32 devices in a mesh: doc: 4 (over y, x), ctx: 8 (over z, core).
Axes of the slice: x: 2, y: 2, z: 4, core: 2. Of those that a mesh axis runs over, the one named last changes fastest.
Arguments:
- summary_cache: bfloat16 [8, 16, 512, 2048], P(None, 'doc', None, 'ctx'), may hold values from -4 to 4
- queries: bfloat16 [4, 2048, 4096], P('doc', 'ctx'), may hold values from -100 to 100
- section_counts: int32 [16], replicated, may hold values from 1 to 2
- summary_blocks: int32 [16, 2], replicated, may hold values from 1 to 2
Outputs:
- attended: bfloat16 [4, 2048, 4096], P('doc', 'ctx')
- relayed: bfloat16 [8, 4, 2048, 2048], P(None, 'doc', 'ctx')
The draws below stay inside these ranges and needn't reach their ends.
All inputs are finite; a program needn't handle non-finite values.
Results may differ from the reference program's by a relative error of at most 0.0045.
Values may be sent and summed in bfloat16 or wider, within the bound.
A program may use at most 192 MiB of HBM per device.

```python
import math
import jax
import jax.numpy as jnp
from jax import lax

QH = 32
KVH = 8
HD = 128
LAYERS = 8
BLOCK = 128
SUMBLK = 2
SECTIONS = 2
GROUP = 4
FEAT = 2048
SUMLEN = 256
SEQD = 512
GROUPS = 4
DOCS = 16
GSEQ = 2048


def draw_summary_cache(key, part):
    array_shape = (LAYERS, DOCS, SEQD, FEAT)
    base_key = jax.random.fold_in(key, 3)
    values = jnp.clip(jax.random.normal(base_key, array_shape, jnp.float32), -4.0, 4.0)
    return values.astype(jnp.bfloat16)


def draw_queries(key, part):
    array_shape = (GROUPS, GSEQ, QH * HD)
    base_key = jax.random.fold_in(key, 5)
    values = jnp.clip(jax.random.normal(base_key, array_shape, jnp.float32), -4.0, 4.0)
    return values.astype(jnp.bfloat16)


def with_ends(values, key, least, largest):
    longest = values.shape.index(max(values.shape))
    spots = []
    for shift in (0, 1):
        where = [jax.random.randint(jax.random.fold_in(key, axis), (), 0, length) for axis, length in enumerate(values.shape)]
        where[longest] = (where[longest] + shift) % values.shape[longest]
        spots.append(tuple(where))
    return values.at[spots[0]].set(least).at[spots[1]].set(largest)


def setup_inputs(seed: int = 0) -> dict:
    arg_keys = jax.random.split(jax.random.key(seed), 5)
    summary_cache = draw_summary_cache(jax.random.fold_in(arg_keys[4], 71), 0)
    queries = draw_queries(jax.random.fold_in(arg_keys[4], 71), 0)
    section_counts = with_ends(jax.random.randint(arg_keys[2], (DOCS,), 1, SECTIONS + 1), jax.random.fold_in(arg_keys[2], 1), 1, SECTIONS).astype(jnp.int32)
    summary_blocks = with_ends(jax.random.randint(arg_keys[3], (DOCS, SECTIONS), 1, SUMBLK + 1), jax.random.fold_in(arg_keys[3], 1), 1, SUMBLK).astype(jnp.int32)
    return dict(summary_cache=summary_cache, queries=queries, section_counts=section_counts, summary_blocks=summary_blocks)


NEGATIVE = -1e+30

def attend_group(operands):
    query_rows, key_rows, validity = operands
    block_rows = min(GSEQ, 512)
    pieces = []
    for offset in range(0, GSEQ, block_rows):
        key_end = offset + block_rows
        grouped = query_rows[offset:key_end].astype(jnp.float32).reshape(block_rows, KVH, GROUP, HD)
        key_heads = key_rows[:key_end, :KVH * HD].astype(jnp.float32).reshape(key_end, KVH, HD)
        value_heads = key_rows[:key_end, KVH * HD:].astype(jnp.float32).reshape(key_end, KVH, HD)
        scores = jnp.einsum('pkgd,skd->kgps', grouped, key_heads) * (1.0 / math.sqrt(HD))
        key_positions = jnp.arange(key_end)
        query_positions = offset + jnp.arange(block_rows)
        allowed = validity[None, :key_end] & (key_positions[None, :] <= query_positions[:, None])
        masked = jnp.where(allowed, scores, NEGATIVE)
        row_maximum = lax.optimization_barrier(jnp.max(masked, axis=-1, keepdims=True))
        weights = jnp.where(allowed, jnp.exp(masked - row_maximum), 0.0)
        denominator = lax.optimization_barrier(jnp.sum(weights, axis=-1))
        rounded = lax.optimization_barrier(weights.astype(jnp.bfloat16)).astype(jnp.float32)
        accumulated = jnp.einsum('kgps,skd->kgpd', rounded, value_heads)
        result = accumulated / denominator[..., None]
        pieces.append(jnp.transpose(result, (2, 0, 1, 3)).reshape(block_rows, QH * HD))
    return jnp.concatenate(pieces, axis=0).astype(jnp.bfloat16)

def reference(summary_cache, queries, section_counts, summary_blocks):
    relayed = jnp.transpose(summary_cache.reshape(LAYERS, GROUPS, GROUPS, SEQD, FEAT), (0, 2, 1, 3, 4)).reshape(LAYERS, GROUPS, GSEQ, FEAT)
    counts_table = jnp.transpose(section_counts.reshape(GROUPS, GROUPS), (1, 0))
    blocks_table = jnp.transpose(summary_blocks.reshape(GROUPS, GROUPS, SECTIONS), (1, 0, 2))
    live_section = jnp.arange(SECTIONS)[None, None, :] < counts_table[:, :, None]
    live_slot = jnp.arange(SUMLEN)[None, None, None, :] < BLOCK * blocks_table[:, :, :, None]
    validity = (live_section[..., None] & live_slot).reshape(GROUPS, GSEQ)
    attended = lax.map(attend_group, (queries, relayed[0], validity))
    return (attended, relayed)
```

```python
import functools
import math

import jax
import jax.numpy as jnp
from jax import lax
from jax.experimental import pallas as pl
from jax.experimental.pallas import tpu as pltpu
from jax.sharding import PartitionSpec as P

QH = 32
KVH = 8
HD = 128
BLOCK = 128
SECTIONS = 2
GROUP = 4
SUMLEN = 256
PARTS = 4


NEGATIVE = -1e30


MESH = pl.DeviceIdType.MESH


def kernel(
    rows,
    ctx,
    cache,
    queries,
    counts,
    blocks,
    attended,
    relayed,
    kv,
    mid,
    stage,
    fwd,
    q_vmem,
    out_vmem,
    bias,
    s1,
    r1_first,
    r1,
    up_sem,
    down_sem,
    side_sem,
    kv_sem,
    s2,
    r2,
    local_sem,
    stage_sem,
    hello,
    fwd_sem,
    s3,
):
    layers, _, slots, feat = cache.shape
    own = queries.shape[0]
    chips = ctx // 2
    parts = kv_sem.shape[2]
    size = slots // parts
    me = lax.axis_index("doc")
    c = lax.axis_index("ctx")
    z = c // 2
    core = c % 2
    binary = rows & (rows - 1) == 0

    def partner(k):
        if not binary:
            return (me + k) % rows
        row, bit = me, 1
        while bit < rows:
            if k & bit:
                row = row + bit * (1 - 2 * ((me // bit) % 2))
            bit *= 2
        return row

    def steps_to(k):
        return bin(k).count("1") if binary else 1

    near = [k for k in range(1, rows) if steps_to(k) == 1]
    rounds = max([steps_to(k) - 1 for k in range(1, rows)])

    def seen(chip):
        return ((2 * chip + 2) * own + slots - 1) // slots

    def greet_rows(sem):
        for k in near:
            pl.semaphore_signal(sem, inc=1, device_id=(partner(k), c), device_id_type=MESH)

    sides = jnp.where(z > 0, 1, 0) + jnp.where(z < chips - 1, 1, 0)
    barrier = pltpu.get_barrier_semaphore()
    for up in (1, -1):

        @pl.when((z + up >= 0) & (z + up < chips))
        def _():
            for other in (core, 1 - core):
                pl.semaphore_signal(barrier, inc=1, device_id=(me, 2 * (z + up) + other), device_id_type=MESH)

    greet_rows(barrier)
    pl.semaphore_signal(barrier, inc=1, device_id=(me, c + 1 - 2 * core), device_id_type=MESH)

    own_kv = pltpu.make_async_copy(
        cache.at[0, me], kv.at[c, pl.ds(pl.multiple_of(me * slots, slots), slots)], local_sem.at[0]
    )
    own_kv.start()

    def staged(k):
        return pltpu.make_async_copy(cache.at[0, partner(k)], stage.at[k - 1], stage_sem.at[k - 1])

    for k in range(1, rows):
        staged(k).start()
    q_copy = pltpu.make_async_copy(queries, q_vmem, local_sem.at[1])
    own_mid = pltpu.make_async_copy(
        cache.at[pl.ds(1, layers - 1), me],
        mid.at[:, pl.ds(pl.multiple_of(me * slots, slots), slots)],
        local_sem.at[2],
    )
    pl.semaphore_wait(barrier, 2 * sides + len(near) + 1)

    def doc(slice_index, j):
        return kv.at[slice_index, pl.ds(pl.multiple_of(j * slots, slots), slots)]

    def part(slice_index, j, h):
        return kv.at[slice_index, pl.ds(pl.multiple_of(j * slots + h * size, size), size)]

    def first_copy(k, j_to, j_from, h):
        return pltpu.make_async_remote_copy(
            src_ref=stage.at[k - 1, pl.ds(h * size, size)],
            dst_ref=part(c, j_from, h),
            send_sem=s1,
            recv_sem=r1_first.at[j_from, h],
            device_id=(j_to, c),
            device_id_type=MESH,
        )

    def row_copy(l, j_to):
        return pltpu.make_async_remote_copy(
            src_ref=cache.at[l, j_to],
            dst_ref=mid.at[l - 1, pl.ds(pl.multiple_of(me * slots, slots), slots)],
            send_sem=s1,
            recv_sem=r1.at[l],
            device_id=(j_to, c),
            device_id_type=MESH,
        )

    def kv_part(slice_index, j, h, sems, target):
        return pltpu.make_async_remote_copy(
            src_ref=part(slice_index, j, h),
            dst_ref=part(slice_index, j, h),
            send_sem=sems.at[slice_index // 2, j],
            recv_sem=kv_sem.at[slice_index, j, h],
            device_id=(me, target),
            device_id_type=MESH,
        )

    def kv_doc(slice_index, j, sems, target):
        return pltpu.make_async_remote_copy(
            src_ref=doc(slice_index, j),
            dst_ref=doc(slice_index, j),
            send_sem=sems.at[slice_index // 2, j],
            recv_sem=kv_sem.at[slice_index, j, 0],
            device_id=(me, target),
            device_id_type=MESH,
        )

    def pass_up(slice_index, j, h):
        @pl.when(z < chips - 1)
        def _():
            kv_part(slice_index, j, h, up_sem, c + 2).start()

    def pass_down(slice_index, j, h):
        @pl.when((z > 0) & (j < seen(z - 1)))
        def _():
            kv_part(slice_index, j, h, down_sem, c - 2).start()

    def pass_side(slice_index, j):
        @pl.when(j < seen(z))
        def _():
            kv_doc(slice_index, j, side_sem, c + 1 - 2 * core).start()

    own_kv.wait()
    for h in range(parts):
        pass_up(c, me, h)
    for k in near:
        staged(k).wait()
    for h in range(parts):
        for k in near:
            first_copy(k, partner(k), me, h).start()
    for h in range(parts):
        pass_down(c, me, h)
    pass_side(c, me)
    own_mid.start()
    q_copy.start()

    for r in range(rounds):
        greet_rows(hello.at[r])
        pl.semaphore_wait(hello.at[r], len(near))
        for k in range(1, rows):
            if steps_to(k) == r + 2:
                staged(k).wait()
                for h in range(parts):
                    first_copy(k, partner(k), me, h).start()

    def from_row(ks):
        for h in range(parts):
            for k in ks:
                j = partner(k)
                first_copy(k, me, j, h).wait_recv()
                pass_up(c, j, h)
                pass_down(c, j, h)
                if h == parts - 1:
                    pass_side(c, j)

    def from_below(step, ks):
        @pl.when(z >= step)
        def _():
            for k in ks:
                j = partner(k)
                for h in range(parts):
                    kv_part(c - 2 * step, j, h, up_sem, c).wait_recv()
                    pass_up(c - 2 * step, j, h)
                pass_side(c - 2 * step, j)

    def from_above(step, ks):
        @pl.when(z + step < chips)
        def _():
            for k in ks:
                j = partner(k)

                @pl.when(j < seen(z))
                def _():
                    for h in range(parts):
                        kv_part(c + 2 * step, j, h, down_sem, c).wait_recv()
                        pass_down(c + 2 * step, j, h)
                    pass_side(c + 2 * step, j)

    both = 2 * own
    half = chips // 2

    def waiting(at, l, s, t):
        ups = at * (chips - 1 - at)
        slot = jnp.where(s < at, s * (chips - 1 - at) + t - at - 1, ups + (s - at - 1) * at + t)
        return fwd.at[l - 1, slot], fwd_sem.at[l - 1, slot]

    def columns(s):
        return pl.ds(pl.multiple_of((2 * s + core) * feat, feat), feat)

    def hop(l, s, m, up, source, sent):
        if m > 1:
            there, arrived = waiting(z + up, l, s, z + up * m)
            pltpu.make_async_remote_copy(
                src_ref=source(0, both),
                dst_ref=there,
                send_sem=sent,
                recv_sem=arrived,
                device_id=(me, c + 2 * up),
                device_id_type=MESH,
            ).start()
        else:
            for other in (core, 1 - core):
                pltpu.make_async_remote_copy(
                    src_ref=source(other * own, own),
                    dst_ref=relayed.at[l, :, columns(s)],
                    send_sem=sent,
                    recv_sem=r2,
                    device_id=(me, 2 * (z + up) + other),
                    device_id_type=MESH,
                ).start()

    def layer_step(l):
        arrived = mid.at[l - 1, pl.ds(0, (rows - 1) * slots)]
        pltpu.make_async_copy(arrived, arrived, r1.at[l]).wait()

        def block(at, length):
            return mid.at[l - 1, pl.ds(pl.multiple_of(at, own), length)]

        for m in range(chips - 1, 0, -1):
            for up in (1, -1):

                @pl.when((z + up * m >= 0) & (z + up * m < chips))
                def _():
                    hop(l, z, m, up, lambda at, length: block((z + up * m) * both + at, length), s2)

        pltpu.make_async_remote_copy(
            src_ref=block(z * both + (1 - core) * own, own),
            dst_ref=relayed.at[l, :, columns(z)],
            send_sem=s2,
            recv_sem=r2,
            device_id=(me, c + 1 - 2 * core),
            device_id_type=MESH,
        ).start()
        pltpu.make_async_copy(block(c * own, own), relayed.at[l, :, columns(z)], local_sem.at[3]).start()

    def forward(ls, late):
        for m in range(chips - 2, 0, -1):
            for l in ls:
                for e in range(1, chips - m):
                    for up in (1, -1):
                        s, t = z - up * e, z + up * m
                        crossed = (s < half) != (z < half)
                        held = (s >= 0) & (s < chips) & (t >= 0) & (t < chips)

                        @pl.when(held & (crossed if late else jnp.logical_not(crossed)))
                        def _():
                            here, arrived = waiting(z, l, s, t)
                            pltpu.make_async_copy(here, here, arrived).wait()
                            hop(l, s, m, up, lambda at, length: here.at[pl.ds(pl.multiple_of(at, own), length)], s3)

    far = [k for k in range(1, rows) if k not in near]
    every = [0] + near + far
    from_row(near)
    from_above(1, [0] + near)
    from_below(1, [0] + near)
    from_row(far)

    @pl.loop(1, layers)
    def _(l):
        for k in range(1, rows):
            row_copy(l, partner(k)).start()

    from_above(1, far)
    own_mid.wait()
    layer_step(1)
    from_below(1, far)
    for step in range(2, chips):
        from_above(step, every)
        if step < layers:
            layer_step(step)
        if step <= layers:
            forward([step - 1], False)
        from_below(step, every)

    events = [[] for _ in range(KVH + 1)]

    def plan(slot, *event):
        events[min(slot, KVH)].append(event)

    following = max(chips, 2)
    for l in range(following, layers):
        plan(l - following, layer_step, l)
    first = max(chips - 1, 1)
    for l in range(first, layers - 2):
        plan(l - first, forward, [l], False)
    last = [l for l in range(layers - 2, layers) if l >= first]
    if last:
        plan(layers - 1 - first, forward, last, False)
    for l in range(1, layers):
        plan(l + 1, forward, [l], True)

    def run(slot):
        for act, *rest in events[slot]:
            act(*rest)

    @pl.loop(0, seen(z))
    def _(j):
        at = j * rows + me
        key = lax.broadcasted_iota(jnp.int32, (own, slots), 1)
        query = lax.broadcasted_iota(jnp.int32, (own, slots), 0)
        section = key // SUMLEN
        reach = jnp.zeros((own, slots), jnp.int32)
        for s in range(SECTIONS):
            reach = jnp.where((section == s) & (s < counts[at]), BLOCK * blocks[s, at], reach)
        allowed = (key - section * SUMLEN < reach) & (j * slots + key <= c * own + query)
        bias[j] = jnp.where(allowed, 0.0, NEGATIVE)

    for other in range(chips):
        slice_index = 2 * other + 1 - core

        @pl.loop(0, seen(z))
        def _(j):
            kv_doc(slice_index, j, side_sem, c).wait_recv()

    q_copy.wait()
    for t in range(ctx):
        pltpu.make_async_copy(
            kv.at[t, pl.ds(pl.multiple_of(c * own, own), own)],
            relayed.at[0, :, pl.ds(t * feat, feat)],
            local_sem.at[4],
        ).start()

    factor = math.log2(math.e) / math.sqrt(HD)

    @pl.loop(0, KVH)
    def _(k):
        for slot in range(KVH):
            if events[slot]:

                @pl.when(k == slot)
                def _():
                    run(slot)

        per = feat // HD
        key_slice = k // per
        value_slice = (KVH + k) // per
        lanes = pl.ds(pl.multiple_of((k % per) * HD, HD), HD)
        for i in range(GROUP):
            column = pl.ds(pl.multiple_of((k * GROUP + i) * HD, HD), HD)
            q = q_vmem[:, column]

            def block(j, state):
                top, total, acc = state
                at = pl.ds(pl.multiple_of(j * slots, slots), slots)
                s = lax.dot_general(
                    q, kv[key_slice, at, lanes], (((1,), (1,)), ((), ())), preferred_element_type=jnp.float32
                )
                s = s + bias[j]
                newest = jnp.maximum(top, jnp.max(s, axis=1, keepdims=True))
                w = jnp.exp2((s - newest) * factor)
                shrink = jnp.exp2((top - newest) * factor)
                total = total * shrink + jnp.sum(w, axis=1, keepdims=True)
                acc = acc * shrink + jnp.dot(
                    w.astype(jnp.bfloat16), kv[value_slice, at, lanes], preferred_element_type=jnp.float32
                )
                return newest, total, acc

            start = (
                jnp.full((own, 1), NEGATIVE, jnp.float32),
                jnp.zeros((own, 1), jnp.float32),
                jnp.zeros((own, HD), jnp.float32),
            )
            _, total, acc = lax.fori_loop(0, seen(z), block, start)
            out_vmem[:, column] = (acc / total).astype(jnp.bfloat16)

    out_copy = pltpu.make_async_copy(out_vmem, attended, local_sem.at[1])
    out_copy.start()
    run(KVH)

    @pl.loop(0, ctx)
    def _(t):
        @pl.loop(0, rows)
        def _(j):
            @pl.when(t % 2 == core)
            def _():
                chip = t // 2

                @pl.when((z < chips - 1) & (chip <= z))
                def _():
                    kv_doc(t, j, up_sem, c).wait_send()

                @pl.when((z > 0) & (j < seen(z - 1)) & (chip >= z))
                def _():
                    kv_doc(t, j, down_sem, c).wait_send()

                @pl.when(j < seen(z))
                def _():
                    kv_doc(t, j, side_sem, c).wait_send()

    def sized(ref, sem):
        return pltpu.make_async_copy(ref, ref, sem)

    sized(cache.at[:, pl.ds(0, rows - 1)], s1).wait()
    passed = relayed.at[pl.ds(1, layers - 1), :, pl.ds(0, (ctx - 1) * feat)]
    sized(passed, s2).wait()
    for q in range(chips):
        kept = 2 * q * (chips - 1 - q)
        if kept:

            @pl.when(z == q)
            def _():
                sized(fwd.at[:, pl.ds(0, kept)], s3).wait()

    sized(passed, r2).wait()
    sized(relayed.at[pl.ds(1, layers - 1), :, pl.ds(0, feat)], local_sem.at[3]).wait()
    sized(relayed.at[0], local_sem.at[4]).wait()
    out_copy.wait()


def copy_out(attended, relayed, attended_out, relayed_out, sems):
    layers = relayed.shape[0]
    copies = [pltpu.make_async_copy(relayed.at[l], relayed_out.at[l], sems.at[l]) for l in range(layers)]
    copies.append(pltpu.make_async_copy(attended, attended_out, sems.at[layers]))
    for copy in copies:
        copy.start()
    for copy in copies:
        copy.wait()


def deliver(attended, relayed):
    any_space = pl.BlockSpec(memory_space=pl.ANY)
    return pl.pallas_call(
        copy_out,
        out_shape=(
            jax.ShapeDtypeStruct(attended.shape, attended.dtype),
            jax.ShapeDtypeStruct(relayed.shape, relayed.dtype),
        ),
        in_specs=[any_space, any_space],
        out_specs=(any_space, any_space),
        scratch_shapes=[pltpu.SemaphoreType.DMA((relayed.shape[0] + 1,))],
        compiler_params=pltpu.CompilerParams(vmem_limit_bytes=4 * 1024 * 1024),
    )(attended, relayed)


def local(summary_cache, queries, section_counts, summary_blocks):
    rows = lax.axis_size("doc")
    ctx = lax.axis_size("ctx")
    layers, documents, slots, feat = summary_cache.shape
    own = queries.shape[1]
    dtype = summary_cache.dtype
    any_space = pl.BlockSpec(memory_space=pl.ANY)
    in_place = pl.BlockSpec(memory_space=pltpu.HBM)
    scalars = pl.BlockSpec(memory_space=pltpu.SMEM)
    dma = pltpu.SemaphoreType.DMA
    size = rows * slots * feat * (ctx + layers) * 2 + own * queries.shape[2] * 4 + rows * own * slots * 4
    edge = (ctx // 2 - 1) // 2
    held = max(2 * edge * (ctx // 2 - 1 - edge), 1)
    size = size + (layers - 1) * held * 4 * own * feat
    room = size + own * (layers * ctx * feat + queries.shape[2]) * 2 + 4 * 1024 * 1024
    place = pltpu.VMEM if room < 60 * 1024 * 1024 else pltpu.HBM

    def in_hbm(array):
        return pltpu.with_memory_space_constraint(array, pltpu.HBM)

    attended, relayed = pl.pallas_call(
        functools.partial(kernel, rows, ctx),
        out_shape=(
            place(queries.shape[1:], dtype),
            place((layers, own, ctx * feat), dtype),
        ),
        in_specs=[in_place, in_place, scalars, scalars],
        out_specs=(any_space, any_space),
        scratch_shapes=[
            pltpu.VMEM((ctx, rows * slots, feat), dtype),
            pltpu.VMEM((layers - 1, rows * slots, feat), dtype),
            pltpu.VMEM((rows - 1, slots, feat), dtype),
            pltpu.VMEM((layers - 1, held, 2 * own, feat), dtype),
            pltpu.VMEM(queries.shape[1:], dtype),
            pltpu.VMEM(queries.shape[1:], dtype),
            pltpu.VMEM((rows, own, slots), jnp.float32),
            dma,
            dma((rows, PARTS)),
            dma((layers,)),
            dma((ctx // 2, rows)),
            dma((ctx // 2, rows)),
            dma((ctx // 2, rows)),
            dma((ctx, rows, PARTS)),
            dma,
            dma,
            dma((5,)),
            dma((rows - 1,)),
            pltpu.SemaphoreType.REGULAR((rows,)),
            dma((layers - 1, held)),
            dma,
        ],
        compiler_params=pltpu.CompilerParams(
            collective_id=0, has_side_effects=True, vmem_limit_bytes=size + 3 * 1024 * 1024
        ),
    )(*(in_hbm(x) for x in (summary_cache, queries[0], section_counts, summary_blocks.T)))
    return deliver(attended[None], relayed[:, None])


def solution(mesh):
    placed = (P(None, "doc", None, "ctx"), P("doc", "ctx", None), P(), P())
    return jax.shard_map(
        local,
        mesh=mesh,
        in_specs=placed,
        out_specs=(P("doc", "ctx", None), P(None, "doc", "ctx", None)),
        check_vma=False,
    )
```

```python
import functools
import math

import jax
import jax.numpy as jnp
from jax import lax
from jax.experimental import pallas as pl
from jax.experimental.pallas import tpu as pltpu
from jax.sharding import PartitionSpec as P

QH = 32
KVH = 8
HD = 128
BLOCK = 128
SECTIONS = 2
GROUP = 4
SUMLEN = 256
PARTS = 2


NEGATIVE = -1e30


MESH = pl.DeviceIdType.MESH


def kernel(
    rows,
    ctx,
    cache,
    queries,
    counts,
    blocks,
    attended,
    relayed,
    kv,
    mid,
    stage,
    fwd,
    q_vmem,
    out_vmem,
    bias,
    s1,
    r1_first,
    r1,
    up_sem,
    down_sem,
    side_sem,
    across_sem,
    part_sem,
    doc_sem,
    s2,
    r2,
    local_sem,
    stage_sem,
    hello,
    fwd_sem,
    s3,
):
    layers, _, slots, feat = cache.shape
    own = queries.shape[0]
    chips = ctx // 2
    parts = part_sem.shape[2]
    size = slots // parts
    me = lax.axis_index("doc")
    c = lax.axis_index("ctx")
    z = c // 2
    core = c % 2
    binary = rows & (rows - 1) == 0

    def partner(k):
        if not binary:
            return (me + k) % rows
        row, bit = me, 1
        while bit < rows:
            if k & bit:
                row = row + bit * (1 - 2 * ((me // bit) % 2))
            bit *= 2
        return row

    def steps_to(k):
        return bin(k).count("1") if binary else 1

    near = [k for k in range(1, rows) if steps_to(k) == 1]
    rounds = max([steps_to(k) - 1 for k in range(1, rows)])

    def seen(chip):
        return ((2 * chip + 2) * own + slots - 1) // slots

    def greet_rows(sem):
        for k in near:
            pl.semaphore_signal(sem, inc=1, device_id=(partner(k), c), device_id_type=MESH)

    sides = jnp.where(z > 0, 1, 0) + jnp.where(z < chips - 1, 1, 0)
    barrier = pltpu.get_barrier_semaphore()
    for up in (1, -1):

        @pl.when((z + up >= 0) & (z + up < chips))
        def _():
            for other in (core, 1 - core):
                pl.semaphore_signal(barrier, inc=1, device_id=(me, 2 * (z + up) + other), device_id_type=MESH)

    greet_rows(barrier)
    pl.semaphore_signal(barrier, inc=1, device_id=(me, c + 1 - 2 * core), device_id_type=MESH)

    own_kv = pltpu.make_async_copy(
        cache.at[0, me], kv.at[c, pl.ds(pl.multiple_of(me * slots, slots), slots)], local_sem.at[0]
    )
    own_kv.start()

    def staged(k):
        return pltpu.make_async_copy(cache.at[0, partner(k)], stage.at[k - 1], stage_sem.at[k - 1])

    for k in range(1, rows):
        staged(k).start()
    q_copy = pltpu.make_async_copy(queries, q_vmem, local_sem.at[1])
    own_mid = pltpu.make_async_copy(
        cache.at[pl.ds(1, layers - 1), me],
        mid.at[:, pl.ds(pl.multiple_of(me * slots, slots), slots)],
        local_sem.at[2],
    )
    pl.semaphore_wait(barrier, 2 * sides + len(near) + 1)

    def doc(slice_index, j):
        return kv.at[slice_index, pl.ds(pl.multiple_of(j * slots, slots), slots)]

    def part(slice_index, j, h):
        return kv.at[slice_index, pl.ds(pl.multiple_of(j * slots + h * size, size), size)]

    def first_copy(k, j_to, j_from, h):
        return pltpu.make_async_remote_copy(
            src_ref=stage.at[k - 1, pl.ds(h * size, size)],
            dst_ref=part(c, j_from, h),
            send_sem=s1,
            recv_sem=r1_first.at[j_from, h],
            device_id=(j_to, c),
            device_id_type=MESH,
        )

    def row_copy(l, j_to):
        return pltpu.make_async_remote_copy(
            src_ref=cache.at[l, j_to],
            dst_ref=mid.at[l - 1, pl.ds(pl.multiple_of(me * slots, slots), slots)],
            send_sem=s1,
            recv_sem=r1.at[l],
            device_id=(j_to, c),
            device_id_type=MESH,
        )

    def kv_copy(slice_index, j, h, sent, arrived, target):
        ref = doc(slice_index, j) if h is None else part(slice_index, j, h)
        return pltpu.make_async_remote_copy(
            src_ref=ref,
            dst_ref=ref,
            send_sem=sent,
            recv_sem=arrived,
            device_id=(me, target),
            device_id_type=MESH,
        )

    early = [0] + near

    def arrival(way, step, k, h):
        if step == 1 and k in early:
            return part_sem.at[way, early.index(k), 0 if h is None else h]
        return doc_sem.at[way, step - 1, k]

    def up_copy(step, k, h):
        return kv_copy(c - 2 * step, partner(k), h, up_sem, arrival(0, step + 1, k, h), c + 2)

    def down_copy(step, k, h):
        return kv_copy(c + 2 * step, partner(k), h, down_sem, arrival(1, step + 1, k, h), c - 2)

    def pass_up(step, k, h):
        if step + 1 < chips:

            @pl.when(z < chips - 1)
            def _():
                up_copy(step, k, h).start()

    def pass_down(step, k, h):
        if step + 1 < chips:

            @pl.when((z > 0) & (partner(k) < seen(z - 1)))
            def _():
                down_copy(step, k, h).start()

    def side_copy(slice_index, j):
        return kv_copy(slice_index, j, None, side_sem, across_sem, c + 1 - 2 * core)

    def pass_side(slice_index, j):
        @pl.when(j < seen(z))
        def _():
            side_copy(slice_index, j).start()

    own_kv.wait()
    for h in range(parts):
        pass_up(0, 0, h)
    for k in near:
        staged(k).wait()
    for h in range(parts):
        for k in near:
            first_copy(k, partner(k), me, h).start()
    for h in range(parts):
        pass_down(0, 0, h)
    pass_side(c, me)
    own_mid.start()
    q_copy.start()

    for r in range(rounds):
        greet_rows(hello.at[r])
        pl.semaphore_wait(hello.at[r], len(near))
        for k in range(1, rows):
            if steps_to(k) == r + 2:
                staged(k).wait()
                for h in range(parts):
                    first_copy(k, partner(k), me, h).start()

    def from_row(ks):
        for h in range(parts):
            for k in ks:
                j = partner(k)
                first_copy(k, me, j, h).wait_recv()
                pass_up(0, k, h)
                pass_down(0, k, h)
                if h == parts - 1:
                    pass_side(c, j)

    def pieces_of(step, k):
        return range(parts) if step == 1 and k in early else [None]

    def from_below(step, ks):
        @pl.when(z >= step)
        def _():
            for k in ks:
                for h in pieces_of(step, k):
                    kv_copy(c - 2 * step, partner(k), h, up_sem, arrival(0, step, k, h), c).wait_recv()
                    pass_up(step, k, h)
                pass_side(c - 2 * step, partner(k))

    def from_above(step, ks):
        @pl.when(z + step < chips)
        def _():
            for k in ks:

                @pl.when(partner(k) < seen(z))
                def _():
                    for h in pieces_of(step, k):
                        kv_copy(c + 2 * step, partner(k), h, down_sem, arrival(1, step, k, h), c).wait_recv()
                        pass_down(step, k, h)
                    pass_side(c + 2 * step, partner(k))

    both = 2 * own
    half = chips // 2

    def waiting(at, l, s, t):
        ups = at * (chips - 1 - at)
        slot = jnp.where(s < at, s * (chips - 1 - at) + t - at - 1, ups + (s - at - 1) * at + t)
        return fwd.at[l - 1, slot], fwd_sem.at[l - 1, slot]

    def columns(s):
        return pl.ds(pl.multiple_of((2 * s + core) * feat, feat), feat)

    def hop(l, s, m, up, source, sent):
        if m > 1:
            there, arrived = waiting(z + up, l, s, z + up * m)
            pltpu.make_async_remote_copy(
                src_ref=source(0, both),
                dst_ref=there,
                send_sem=sent,
                recv_sem=arrived,
                device_id=(me, c + 2 * up),
                device_id_type=MESH,
            ).start()
        else:
            for other in (core, 1 - core):
                pltpu.make_async_remote_copy(
                    src_ref=source(other * own, own),
                    dst_ref=relayed.at[l, :, columns(s)],
                    send_sem=sent,
                    recv_sem=r2,
                    device_id=(me, 2 * (z + up) + other),
                    device_id_type=MESH,
                ).start()

    def layer_step(l):
        arrived = mid.at[l - 1, pl.ds(0, (rows - 1) * slots)]
        pltpu.make_async_copy(arrived, arrived, r1.at[l]).wait()

        def block(at, length):
            return mid.at[l - 1, pl.ds(pl.multiple_of(at, own), length)]

        for m in range(chips - 1, 0, -1):
            for up in (1, -1):

                @pl.when((z + up * m >= 0) & (z + up * m < chips))
                def _():
                    hop(l, z, m, up, lambda at, length: block((z + up * m) * both + at, length), s2)

        pltpu.make_async_remote_copy(
            src_ref=block(z * both + (1 - core) * own, own),
            dst_ref=relayed.at[l, :, columns(z)],
            send_sem=s2,
            recv_sem=r2,
            device_id=(me, c + 1 - 2 * core),
            device_id_type=MESH,
        ).start()
        pltpu.make_async_copy(block(c * own, own), relayed.at[l, :, columns(z)], local_sem.at[3]).start()

    def forward(ls, hops, late):
        for m in range(chips - 2, 0, -1):
            for l in ls:
                for e in hops:
                    if e + m > chips - 1:
                        continue
                    for up in (1, -1):
                        s, t = z - up * e, z + up * m
                        crossed = (s < half) != (z < half)
                        held = (s >= 0) & (s < chips) & (t >= 0) & (t < chips)

                        @pl.when(held & (crossed if late else jnp.logical_not(crossed)))
                        def _():
                            here, arrived = waiting(z, l, s, t)
                            pltpu.make_async_copy(here, here, arrived).wait()
                            hop(l, s, m, up, lambda at, length: here.at[pl.ds(pl.multiple_of(at, own), length)], s3)

    far = [k for k in range(1, rows) if k not in near]
    every = early + far
    hops = range(1, chips - 1)
    from_row(near)
    from_above(1, early)
    from_below(1, early)
    from_row(far)

    @pl.loop(1, layers)
    def _(l):
        for k in range(1, rows):
            row_copy(l, partner(k)).start()

    from_above(1, far)
    own_mid.wait()
    layer_step(1)
    from_below(1, far)
    for step in range(2, chips):
        from_above(step, every)
        if step < layers:
            layer_step(step)
        if step <= layers:
            forward([step - 1], hops, False)
        from_below(step, every)

    events = [[] for _ in range(KVH + 1)]

    def plan(slot, *event):
        events[min(slot, KVH)].append(event)

    following = max(chips, 2)
    first = max(chips - 1, 1)
    last = [l for l in range(layers - 2, layers) if l >= first]
    late = sorted((l + 2 * e, -e) for l in range(1, layers) for e in hops)
    for l in range(following, layers):
        plan(l - following, layer_step, l)
    for total, e in late:
        if e < -1:
            plan(max(0, (total - 4) * 4 // 3), forward, [total + 2 * e], [-e], True)
    for l in range(first, layers - 2):
        plan(l - first + 1, forward, [l], hops, False)
    if last:
        plan(layers - 2, forward, last, hops, False)
    for total, e in late:
        if e == -1:
            plan(max(0, (total - 4) * 4 // 3), forward, [total - 2], [1], True)

    def run(slot):
        for act, *rest in events[slot]:
            act(*rest)

    @pl.loop(0, seen(z))
    def _(j):
        at = j * rows + me
        key = lax.broadcasted_iota(jnp.int32, (own, slots), 1)
        query = lax.broadcasted_iota(jnp.int32, (own, slots), 0)
        section = key // SUMLEN
        reach = jnp.zeros((own, slots), jnp.int32)
        for s in range(SECTIONS):
            reach = jnp.where((section == s) & (s < counts[at]), BLOCK * blocks[s, at], reach)
        allowed = (key - section * SUMLEN < reach) & (j * slots + key <= c * own + query)
        bias[j] = jnp.where(allowed, 0.0, NEGATIVE)

    def sized(ref, sem):
        return pltpu.make_async_copy(ref, ref, sem)

    for q in range(chips):

        @pl.when(z == q)
        def _():
            sized(kv.at[pl.ds(0, chips), pl.ds(0, seen(q) * slots)], across_sem).wait()

    q_copy.wait()
    for t in range(ctx):
        pltpu.make_async_copy(
            kv.at[t, pl.ds(pl.multiple_of(c * own, own), own)],
            relayed.at[0, :, pl.ds(t * feat, feat)],
            local_sem.at[4],
        ).start()

    factor = math.log2(math.e) / math.sqrt(HD)

    @pl.loop(0, KVH)
    def _(k):
        for slot in range(KVH):
            if events[slot]:

                @pl.when(k == slot)
                def _():
                    run(slot)

        per = feat // HD
        key_slice = k // per
        value_slice = (KVH + k) // per
        lanes = pl.ds(pl.multiple_of((k % per) * HD, HD), HD)
        for i in range(GROUP):
            column = pl.ds(pl.multiple_of((k * GROUP + i) * HD, HD), HD)
            q = q_vmem[:, column]

            def block(j, state):
                top, total, acc = state
                at = pl.ds(pl.multiple_of(j * slots, slots), slots)
                s = lax.dot_general(
                    q, kv[key_slice, at, lanes], (((1,), (1,)), ((), ())), preferred_element_type=jnp.float32
                )
                s = s + bias[j]
                newest = jnp.maximum(top, jnp.max(s, axis=1, keepdims=True))
                w = jnp.exp2((s - newest) * factor)
                shrink = jnp.exp2((top - newest) * factor)
                total = total * shrink + jnp.sum(w, axis=1, keepdims=True)
                acc = acc * shrink + jnp.dot(
                    w.astype(jnp.bfloat16), kv[value_slice, at, lanes], preferred_element_type=jnp.float32
                )
                return newest, total, acc

            start = (
                jnp.full((own, 1), NEGATIVE, jnp.float32),
                jnp.zeros((own, 1), jnp.float32),
                jnp.zeros((own, HD), jnp.float32),
            )
            _, total, acc = lax.fori_loop(0, seen(z), block, start)
            out_vmem[:, column] = (acc / total).astype(jnp.bfloat16)

    out_copy = pltpu.make_async_copy(out_vmem, attended, local_sem.at[1])
    out_copy.start()
    run(KVH)

    for q in range(chips):

        @pl.when(z == q)
        def _():
            if q < chips - 1:
                sized(kv.at[pl.ds(0, q + 1)], up_sem).wait()
            if q > 0:
                sized(kv.at[pl.ds(0, chips - q), pl.ds(0, seen(q - 1) * slots)], down_sem).wait()
            sized(kv.at[pl.ds(0, chips), pl.ds(0, seen(q) * slots)], side_sem).wait()

    sized(cache.at[:, pl.ds(0, rows - 1)], s1).wait()
    passed = relayed.at[pl.ds(1, layers - 1), :, pl.ds(0, (ctx - 1) * feat)]
    sized(passed, s2).wait()
    for q in range(chips):
        kept = 2 * q * (chips - 1 - q)
        if kept:

            @pl.when(z == q)
            def _():
                sized(fwd.at[:, pl.ds(0, kept)], s3).wait()

    sized(passed, r2).wait()
    sized(relayed.at[pl.ds(1, layers - 1), :, pl.ds(0, feat)], local_sem.at[3]).wait()
    sized(relayed.at[0], local_sem.at[4]).wait()
    out_copy.wait()


def copy_out(attended, relayed, attended_out, relayed_out, sems):
    layers = relayed.shape[0]
    copies = [pltpu.make_async_copy(relayed.at[l], relayed_out.at[l], sems.at[l]) for l in range(layers)]
    copies.append(pltpu.make_async_copy(attended, attended_out, sems.at[layers]))
    for copy in copies:
        copy.start()
    for copy in copies:
        copy.wait()


def deliver(attended, relayed):
    any_space = pl.BlockSpec(memory_space=pl.ANY)
    return pl.pallas_call(
        copy_out,
        out_shape=(
            jax.ShapeDtypeStruct(attended.shape, attended.dtype),
            jax.ShapeDtypeStruct(relayed.shape, relayed.dtype),
        ),
        in_specs=[any_space, any_space],
        out_specs=(any_space, any_space),
        scratch_shapes=[pltpu.SemaphoreType.DMA((relayed.shape[0] + 1,))],
        compiler_params=pltpu.CompilerParams(vmem_limit_bytes=4 * 1024 * 1024),
    )(attended, relayed)


def local(summary_cache, queries, section_counts, summary_blocks):
    rows = lax.axis_size("doc")
    ctx = lax.axis_size("ctx")
    layers, documents, slots, feat = summary_cache.shape
    own = queries.shape[1]
    dtype = summary_cache.dtype
    any_space = pl.BlockSpec(memory_space=pl.ANY)
    in_place = pl.BlockSpec(memory_space=pltpu.HBM)
    scalars = pl.BlockSpec(memory_space=pltpu.SMEM)
    dma = pltpu.SemaphoreType.DMA
    size = rows * slots * feat * (ctx + layers) * 2 + own * queries.shape[2] * 4 + rows * own * slots * 4
    edge = (ctx // 2 - 1) // 2
    held = max(2 * edge * (ctx // 2 - 1 - edge), 1)
    size = size + (layers - 1) * held * 4 * own * feat
    room = size + own * (layers * ctx * feat + queries.shape[2]) * 2 + 4 * 1024 * 1024
    place = pltpu.VMEM if room < 60 * 1024 * 1024 else pltpu.HBM

    def in_hbm(array):
        return pltpu.with_memory_space_constraint(array, pltpu.HBM)

    attended, relayed = pl.pallas_call(
        functools.partial(kernel, rows, ctx),
        out_shape=(
            place(queries.shape[1:], dtype),
            place((layers, own, ctx * feat), dtype),
        ),
        in_specs=[in_place, in_place, scalars, scalars],
        out_specs=(any_space, any_space),
        scratch_shapes=[
            pltpu.VMEM((ctx, rows * slots, feat), dtype),
            pltpu.VMEM((layers - 1, rows * slots, feat), dtype),
            pltpu.VMEM((rows - 1, slots, feat), dtype),
            pltpu.VMEM((layers - 1, held, 2 * own, feat), dtype),
            pltpu.VMEM(queries.shape[1:], dtype),
            pltpu.VMEM(queries.shape[1:], dtype),
            pltpu.VMEM((rows, own, slots), jnp.float32),
            dma,
            dma((rows, PARTS)),
            dma((layers,)),
            dma,
            dma,
            dma,
            dma,
            dma((2, rows, PARTS)),
            dma((2, max(ctx // 2 - 1, 1), rows)),
            dma,
            dma,
            dma((5,)),
            dma((rows - 1,)),
            pltpu.SemaphoreType.REGULAR((max(rows.bit_length() - 2, 1),)),
            dma((layers - 1, held)),
            dma,
        ],
        compiler_params=pltpu.CompilerParams(
            collective_id=0, has_side_effects=True, vmem_limit_bytes=size + 3 * 1024 * 1024
        ),
    )(*(in_hbm(x) for x in (summary_cache, queries[0], section_counts, summary_blocks.T)))
    return deliver(attended[None], relayed[:, None])


def solution(mesh):
    placed = (P(None, "doc", None, "ctx"), P("doc", "ctx", None), P(), P())
    return jax.shard_map(
        local,
        mesh=mesh,
        in_specs=placed,
        out_specs=(P("doc", "ctx", None), P(None, "doc", "ctx", None)),
        check_vma=False,
    )
```

```python
import functools
import math

import jax
import jax.numpy as jnp
from jax import lax
from jax.experimental import pallas as pl
from jax.experimental.pallas import tpu as pltpu
from jax.sharding import PartitionSpec as P

QH = 32
KVH = 8
HD = 128
BLOCK = 128
SECTIONS = 2
GROUP = 4
SUMLEN = 256
PARTS = 2


NEGATIVE = -1e30


MESH = pl.DeviceIdType.MESH


def kernel(
    rows,
    ctx,
    cache,
    queries,
    counts_in,
    blocks_in,
    attended,
    relayed,
    kv,
    mid,
    stage,
    fwd,
    q_vmem,
    out_vmem,
    bias,
    s1,
    r1_first,
    r1,
    up_sem,
    down_sem,
    side_sem,
    across_sem,
    part_sem,
    doc_sem,
    s2,
    r2,
    local_sem,
    stage_sem,
    hello,
    fwd_sem,
    s3,
    counts,
    blocks,
    table_sem,
):
    layers, _, slots, feat = cache.shape
    own = queries.shape[0]
    chips = ctx // 2
    parts = part_sem.shape[2]
    size = slots // parts
    me = lax.axis_index("doc")
    c = lax.axis_index("ctx")
    z = c // 2
    core = c % 2
    binary = rows & (rows - 1) == 0

    def partner(k):
        if not binary:
            return (me + k) % rows
        row, bit = me, 1
        while bit < rows:
            if k & bit:
                row = row + bit * (1 - 2 * ((me // bit) % 2))
            bit *= 2
        return row

    def steps_to(k):
        return bin(k).count("1") if binary else 1

    near = [k for k in range(1, rows) if steps_to(k) == 1]
    rounds = max([steps_to(k) - 1 for k in range(1, rows)])

    def seen(chip):
        return ((2 * chip + 2) * own + slots - 1) // slots

    def greet_rows(sem):
        for k in near:
            pl.semaphore_signal(sem, inc=1, device_id=(partner(k), c), device_id_type=MESH)

    sides = jnp.where(z > 0, 1, 0) + jnp.where(z < chips - 1, 1, 0)
    barrier = pltpu.get_barrier_semaphore()
    for up in (1, -1):

        @pl.when((z + up >= 0) & (z + up < chips))
        def _():
            for other in (core, 1 - core):
                pl.semaphore_signal(barrier, inc=1, device_id=(me, 2 * (z + up) + other), device_id_type=MESH)

    greet_rows(barrier)
    pl.semaphore_signal(barrier, inc=1, device_id=(me, c + 1 - 2 * core), device_id_type=MESH)

    own_kv = pltpu.make_async_copy(
        cache.at[0, me], kv.at[c, pl.ds(pl.multiple_of(me * slots, slots), slots)], local_sem.at[0]
    )
    own_kv.start()

    def staged(k):
        return pltpu.make_async_copy(cache.at[0, partner(k)], stage.at[k - 1], stage_sem.at[k - 1])

    for k in range(1, rows):
        staged(k).start()
    q_copy = pltpu.make_async_copy(queries, q_vmem, local_sem.at[1])
    own_mid = pltpu.make_async_copy(
        cache.at[pl.ds(1, layers - 1), me],
        mid.at[:, pl.ds(pl.multiple_of(me * slots, slots), slots)],
        local_sem.at[2],
    )
    tables = [
        pltpu.make_async_copy(counts_in, counts, table_sem.at[0]),
        pltpu.make_async_copy(blocks_in, blocks, table_sem.at[1]),
    ]
    for copy in tables:
        copy.start()
    pl.semaphore_wait(barrier, 2 * sides + len(near) + 1)

    def doc(slice_index, j):
        return kv.at[slice_index, pl.ds(pl.multiple_of(j * slots, slots), slots)]

    def part(slice_index, j, h):
        return kv.at[slice_index, pl.ds(pl.multiple_of(j * slots + h * size, size), size)]

    def first_copy(k, j_to, j_from, h):
        return pltpu.make_async_remote_copy(
            src_ref=stage.at[k - 1, pl.ds(h * size, size)],
            dst_ref=part(c, j_from, h),
            send_sem=s1,
            recv_sem=r1_first.at[j_from, h],
            device_id=(j_to, c),
            device_id_type=MESH,
        )

    def row_copy(l, j_to):
        return pltpu.make_async_remote_copy(
            src_ref=cache.at[l, j_to],
            dst_ref=mid.at[l - 1, pl.ds(pl.multiple_of(me * slots, slots), slots)],
            send_sem=s1,
            recv_sem=r1.at[l],
            device_id=(j_to, c),
            device_id_type=MESH,
        )

    def kv_copy(slice_index, j, h, sent, arrived, target):
        ref = doc(slice_index, j) if h is None else part(slice_index, j, h)
        return pltpu.make_async_remote_copy(
            src_ref=ref,
            dst_ref=ref,
            send_sem=sent,
            recv_sem=arrived,
            device_id=(me, target),
            device_id_type=MESH,
        )

    early = [0] + near

    def arrival(way, step, k, h):
        if step == 1 and k in early:
            return part_sem.at[way, early.index(k), 0 if h is None else h]
        return doc_sem.at[way, step - 1, k]

    def up_copy(step, k, h):
        return kv_copy(c - 2 * step, partner(k), h, up_sem, arrival(0, step + 1, k, h), c + 2)

    def down_copy(step, k, h):
        return kv_copy(c + 2 * step, partner(k), h, down_sem, arrival(1, step + 1, k, h), c - 2)

    def pass_up(step, k, h):
        if step + 1 < chips:

            @pl.when(z < chips - 1)
            def _():
                up_copy(step, k, h).start()

    def pass_down(step, k, h):
        if step + 1 < chips:

            @pl.when((z > 0) & (partner(k) < seen(z - 1)))
            def _():
                down_copy(step, k, h).start()

    def side_copy(slice_index, j):
        return kv_copy(slice_index, j, None, side_sem, across_sem, c + 1 - 2 * core)

    def pass_side(slice_index, j):
        @pl.when(j < seen(z))
        def _():
            side_copy(slice_index, j).start()

    own_kv.wait()
    for h in range(parts):
        pass_up(0, 0, h)
    for k in near:
        staged(k).wait()
    for h in range(parts):
        for k in near:
            first_copy(k, partner(k), me, h).start()
    for h in range(parts):
        pass_down(0, 0, h)
    pass_side(c, me)
    own_mid.start()
    q_copy.start()

    for r in range(rounds):
        greet_rows(hello.at[r])
        pl.semaphore_wait(hello.at[r], len(near))
        for k in range(1, rows):
            if steps_to(k) == r + 2:
                staged(k).wait()
                for h in range(parts):
                    first_copy(k, partner(k), me, h).start()

    def from_row(ks):
        for h in range(parts):
            for k in ks:
                j = partner(k)
                first_copy(k, me, j, h).wait_recv()
                pass_up(0, k, h)
                pass_down(0, k, h)
                if h == parts - 1:
                    pass_side(c, j)

    def pieces_of(step, k):
        return range(parts) if step == 1 and k in early else [None]

    def from_below(step, ks):
        @pl.when(z >= step)
        def _():
            for k in ks:
                for h in pieces_of(step, k):
                    kv_copy(c - 2 * step, partner(k), h, up_sem, arrival(0, step, k, h), c).wait_recv()
                    pass_up(step, k, h)
                pass_side(c - 2 * step, partner(k))

    def from_above(step, ks):
        @pl.when(z + step < chips)
        def _():
            for k in ks:

                @pl.when(partner(k) < seen(z))
                def _():
                    for h in pieces_of(step, k):
                        kv_copy(c + 2 * step, partner(k), h, down_sem, arrival(1, step, k, h), c).wait_recv()
                        pass_down(step, k, h)
                    pass_side(c + 2 * step, partner(k))

    both = 2 * own
    half = chips // 2

    def waiting(at, l, s, t):
        ups = at * (chips - 1 - at)
        slot = jnp.where(s < at, s * (chips - 1 - at) + t - at - 1, ups + (s - at - 1) * at + t)
        return fwd.at[l - 1, slot], fwd_sem.at[l - 1, slot]

    def columns(s):
        return pl.ds(pl.multiple_of((2 * s + core) * feat, feat), feat)

    def hop(l, s, m, up, source, sent):
        if m > 1:
            there, arrived = waiting(z + up, l, s, z + up * m)
            pltpu.make_async_remote_copy(
                src_ref=source(0, both),
                dst_ref=there,
                send_sem=sent,
                recv_sem=arrived,
                device_id=(me, c + 2 * up),
                device_id_type=MESH,
            ).start()
        else:
            for other in (core, 1 - core):
                pltpu.make_async_remote_copy(
                    src_ref=source(other * own, own),
                    dst_ref=relayed.at[l, :, columns(s)],
                    send_sem=sent,
                    recv_sem=r2,
                    device_id=(me, 2 * (z + up) + other),
                    device_id_type=MESH,
                ).start()

    def layer_step(l):
        arrived = mid.at[l - 1, pl.ds(0, (rows - 1) * slots)]
        pltpu.make_async_copy(arrived, arrived, r1.at[l]).wait()

        def block(at, length):
            return mid.at[l - 1, pl.ds(pl.multiple_of(at, own), length)]

        for m in range(chips - 1, 0, -1):
            for up in (1, -1):

                @pl.when((z + up * m >= 0) & (z + up * m < chips))
                def _():
                    hop(l, z, m, up, lambda at, length: block((z + up * m) * both + at, length), s2)

        pltpu.make_async_remote_copy(
            src_ref=block(z * both + (1 - core) * own, own),
            dst_ref=relayed.at[l, :, columns(z)],
            send_sem=s2,
            recv_sem=r2,
            device_id=(me, c + 1 - 2 * core),
            device_id_type=MESH,
        ).start()
        pltpu.make_async_copy(block(c * own, own), relayed.at[l, :, columns(z)], local_sem.at[3]).start()

    def forward(ls, hops, late):
        for m in range(chips - 2, 0, -1):
            for l in ls:
                for e in hops:
                    if e + m > chips - 1:
                        continue
                    for up in (1, -1):
                        s, t = z - up * e, z + up * m
                        crossed = (s < half) != (z < half)
                        held = (s >= 0) & (s < chips) & (t >= 0) & (t < chips)

                        @pl.when(held & (crossed if late else jnp.logical_not(crossed)))
                        def _():
                            here, arrived = waiting(z, l, s, t)
                            pltpu.make_async_copy(here, here, arrived).wait()
                            hop(l, s, m, up, lambda at, length: here.at[pl.ds(pl.multiple_of(at, own), length)], s3)

    far = [k for k in range(1, rows) if k not in near]
    every = early + far
    hops = range(1, chips - 1)
    from_row(near)
    from_above(1, early)
    from_below(1, early)
    from_row(far)

    @pl.loop(1, layers)
    def _(l):
        for k in range(1, rows):
            row_copy(l, partner(k)).start()

    from_above(1, far)
    own_mid.wait()
    layer_step(1)
    from_below(1, far)
    for step in range(2, chips):
        from_above(step, every)
        if step < layers:
            layer_step(step)
        if step <= layers:
            forward([step - 1], hops, False)
        from_below(step, every)

    events = [[] for _ in range(KVH + 1)]

    def plan(slot, *event):
        events[min(slot, KVH)].append(event)

    following = max(chips, 2)
    first = max(chips - 1, 1)
    last = [l for l in range(layers - 2, layers) if l >= first]
    late = sorted((l + 2 * e, -e) for l in range(1, layers) for e in hops)
    for l in range(following, layers):
        plan(l - following, layer_step, l)
    for total, e in late:
        if e < -1:
            plan(max(0, (total - 4) * 4 // 3), forward, [total + 2 * e], [-e], True)
    for l in range(first, layers - 2):
        plan(l - first + 1, forward, [l], hops, False)
    if last:
        plan(layers - 2, forward, last, hops, False)
    for total, e in late:
        if e == -1:
            plan(max(0, (total - 4) * 4 // 3), forward, [total - 2], [1], True)

    def run(slot):
        for act, *rest in events[slot]:
            act(*rest)

    for copy in tables:
        copy.wait()

    @pl.loop(0, seen(z))
    def _(j):
        at = j * rows + me
        key = lax.broadcasted_iota(jnp.int32, (own, slots), 1)
        query = lax.broadcasted_iota(jnp.int32, (own, slots), 0)
        section = key // SUMLEN
        reach = jnp.zeros((own, slots), jnp.int32)
        for s in range(SECTIONS):
            reach = jnp.where((section == s) & (s < counts[at]), BLOCK * blocks[s, at], reach)
        allowed = (key - section * SUMLEN < reach) & (j * slots + key <= c * own + query)
        bias[j] = jnp.where(allowed, 0.0, NEGATIVE)

    def sized(ref, sem):
        return pltpu.make_async_copy(ref, ref, sem)

    for q in range(chips):

        @pl.when(z == q)
        def _():
            sized(kv.at[pl.ds(0, chips), pl.ds(0, seen(q) * slots)], across_sem).wait()

    q_copy.wait()
    for t in range(ctx):
        pltpu.make_async_copy(
            kv.at[t, pl.ds(pl.multiple_of(c * own, own), own)],
            relayed.at[0, :, pl.ds(t * feat, feat)],
            local_sem.at[4],
        ).start()

    factor = math.log2(math.e) / math.sqrt(HD)

    @pl.loop(0, KVH)
    def _(k):
        for slot in range(KVH):
            if events[slot]:

                @pl.when(k == slot)
                def _():
                    run(slot)

        per = feat // HD
        key_slice = k // per
        value_slice = (KVH + k) // per
        lanes = pl.ds(pl.multiple_of((k % per) * HD, HD), HD)
        for i in range(GROUP):
            column = pl.ds(pl.multiple_of((k * GROUP + i) * HD, HD), HD)
            q = q_vmem[:, column]

            def block(j, state):
                top, total, acc = state
                at = pl.ds(pl.multiple_of(j * slots, slots), slots)
                s = lax.dot_general(
                    q, kv[key_slice, at, lanes], (((1,), (1,)), ((), ())), preferred_element_type=jnp.float32
                )
                s = s + bias[j]
                newest = jnp.maximum(top, jnp.max(s, axis=1, keepdims=True))
                w = jnp.exp2((s - newest) * factor)
                shrink = jnp.exp2((top - newest) * factor)
                total = total * shrink + jnp.sum(w, axis=1, keepdims=True)
                acc = acc * shrink + jnp.dot(
                    w.astype(jnp.bfloat16), kv[value_slice, at, lanes], preferred_element_type=jnp.float32
                )
                return newest, total, acc

            start = (
                jnp.full((own, 1), NEGATIVE, jnp.float32),
                jnp.zeros((own, 1), jnp.float32),
                jnp.zeros((own, HD), jnp.float32),
            )
            _, total, acc = lax.fori_loop(0, seen(z), block, start)
            out_vmem[:, column] = (acc / total).astype(jnp.bfloat16)

    out_copy = pltpu.make_async_copy(out_vmem, attended, local_sem.at[1])
    out_copy.start()
    run(KVH)

    for q in range(chips):

        @pl.when(z == q)
        def _():
            if q < chips - 1:
                sized(kv.at[pl.ds(0, q + 1)], up_sem).wait()
            if q > 0:
                sized(kv.at[pl.ds(0, chips - q), pl.ds(0, seen(q - 1) * slots)], down_sem).wait()
            sized(kv.at[pl.ds(0, chips), pl.ds(0, seen(q) * slots)], side_sem).wait()

    sized(cache.at[:, pl.ds(0, rows - 1)], s1).wait()
    passed = relayed.at[pl.ds(1, layers - 1), :, pl.ds(0, (ctx - 1) * feat)]
    sized(passed, s2).wait()
    for q in range(chips):
        kept = 2 * q * (chips - 1 - q)
        if kept:

            @pl.when(z == q)
            def _():
                sized(fwd.at[:, pl.ds(0, kept)], s3).wait()

    sized(passed, r2).wait()
    sized(relayed.at[pl.ds(1, layers - 1), :, pl.ds(0, feat)], local_sem.at[3]).wait()
    sized(relayed.at[0], local_sem.at[4]).wait()
    out_copy.wait()


def copy_out(attended, relayed, attended_out, relayed_out, sems):
    for l in range(relayed.shape[0]):
        for h in range(2):
            rows = pl.ds(h * relayed.shape[2] // 2, relayed.shape[2] // 2)
            pltpu.make_async_copy(relayed.at[l, :, rows], relayed_out.at[l, :, rows], sems.at[1]).start()
    for h in range(4):
        rows = pl.ds(h * attended.shape[1] // 4, attended.shape[1] // 4)
        pltpu.make_async_copy(attended.at[:, rows], attended_out.at[:, rows], sems.at[0]).start()
    pltpu.make_async_copy(attended, attended_out, sems.at[0]).wait()
    pltpu.make_async_copy(relayed, relayed_out, sems.at[1]).wait()


def deliver(attended, relayed):
    any_space = pl.BlockSpec(memory_space=pl.ANY)
    return pl.pallas_call(
        copy_out,
        out_shape=(
            jax.ShapeDtypeStruct(attended.shape, attended.dtype),
            jax.ShapeDtypeStruct(relayed.shape, relayed.dtype),
        ),
        in_specs=[any_space, any_space],
        out_specs=(any_space, any_space),
        scratch_shapes=[pltpu.SemaphoreType.DMA((2,))],
        compiler_params=pltpu.CompilerParams(vmem_limit_bytes=4 * 1024 * 1024),
    )(attended, relayed)


def local(summary_cache, queries, section_counts, summary_blocks):
    rows = lax.axis_size("doc")
    ctx = lax.axis_size("ctx")
    layers, documents, slots, feat = summary_cache.shape
    own = queries.shape[1]
    dtype = summary_cache.dtype
    any_space = pl.BlockSpec(memory_space=pl.ANY)
    in_place = pl.BlockSpec(memory_space=pltpu.HBM)
    dma = pltpu.SemaphoreType.DMA
    size = rows * slots * feat * (ctx + layers) * 2 + own * queries.shape[2] * 4 + rows * own * slots * 4
    edge = (ctx // 2 - 1) // 2
    held = max(2 * edge * (ctx // 2 - 1 - edge), 1)
    size = size + (layers - 1) * held * 4 * own * feat
    room = size + own * (layers * ctx * feat + queries.shape[2]) * 2 + 4 * 1024 * 1024
    place = pltpu.VMEM if room < 60 * 1024 * 1024 else pltpu.HBM

    def in_hbm(array):
        return pltpu.with_memory_space_constraint(array, pltpu.HBM)

    attended, relayed = pl.pallas_call(
        functools.partial(kernel, rows, ctx),
        out_shape=(
            place(queries.shape[1:], dtype),
            place((layers, own, ctx * feat), dtype),
        ),
        in_specs=[in_place] * 4,
        out_specs=(any_space, any_space),
        scratch_shapes=[
            pltpu.VMEM((ctx, rows * slots, feat), dtype),
            pltpu.VMEM((layers - 1, rows * slots, feat), dtype),
            pltpu.VMEM((rows - 1, slots, feat), dtype),
            pltpu.VMEM((layers - 1, held, 2 * own, feat), dtype),
            pltpu.VMEM(queries.shape[1:], dtype),
            pltpu.VMEM(queries.shape[1:], dtype),
            pltpu.VMEM((rows, own, slots), jnp.float32),
            dma,
            dma((rows, PARTS)),
            dma((layers,)),
            dma,
            dma,
            dma,
            dma,
            dma((2, rows, PARTS)),
            dma((2, max(ctx // 2 - 1, 1), rows)),
            dma,
            dma,
            dma((5,)),
            dma((rows - 1,)),
            pltpu.SemaphoreType.REGULAR((max(rows.bit_length() - 2, 1),)),
            dma((layers - 1, held)),
            dma,
            pltpu.SMEM(section_counts.shape, jnp.int32),
            pltpu.SMEM(summary_blocks.shape[::-1], jnp.int32),
            dma((2,)),
        ],
        compiler_params=pltpu.CompilerParams(
            collective_id=0, has_side_effects=True, vmem_limit_bytes=size + 3 * 1024 * 1024
        ),
    )(*(in_hbm(x) for x in (summary_cache, queries[0], section_counts, summary_blocks.T)))
    return deliver(attended[None], relayed[:, None])


def solution(mesh):
    placed = (P(None, "doc", None, "ctx"), P("doc", "ctx", None), P(), P())
    return jax.shard_map(
        local,
        mesh=mesh,
        in_specs=placed,
        out_specs=(P("doc", "ctx", None), P(None, "doc", "ctx", None)),
        check_vma=False,
    )
```
